1024 devices in a mesh: energy: 64 (over z, core), ribbon: 16 (over y, x).
Axes of the slice: x: 4, y: 4, z: 32, core: 2. Of those that a mesh axis runs over, the one named last changes fastest.
Arguments:
- transfer: float32 [64, 16, 2, 256, 256], P('energy', 'ribbon'), may hold values from -1.25 to 1.25
- source: float32 [64, 16, 2, 256, 256], P('energy', 'ribbon'), may hold values from -6 to 6
- coulomb: float32 [16, 256, 256], P('ribbon'), may hold values from -6 to 6
Outputs:
- lesser: float32 [64, 16, 2, 256, 256], P('energy', 'ribbon')
- screened: float32 [64, 16, 2, 256, 256], P('energy', 'ribbon')
The draws below stay inside these ranges and needn't reach their ends.
All inputs are finite; a program needn't handle non-finite values.
Results may differ from the reference program's by a relative error of at most 0.0001.
Values sent between devices are 32-bit elements; how exact they have to be, the bound alone decides.
No kernel may reach another device: no remote copies, remote signals or barrier semaphores. Data moves between devices by JAX's collectives and lax.ppermute only.
A program may use at most 64 MiB of HBM per device.

```python
import jax
import jax.numpy as jnp
from jax import lax

M = 256
NE = 64
NB = 16


def draw_transfer(key, part):
    keys = jax.random.split(jax.random.fold_in(key, 7), 5)
    slowest = jnp.sqrt(jnp.float32(0.1) ** (1.0 / NB) - 0.04)
    lowest = jnp.log(jnp.float32(0.3))
    rates = jnp.exp(jax.random.uniform(keys[0], (NE, NB, M), jnp.float32, lowest, jnp.log(slowest)))
    hits = jax.random.uniform(keys[1], (NE, NB, 1), jnp.float32) < 0.2
    factor = jax.random.uniform(keys[2], (NE, NB, 1), jnp.float32, 0.7, 0.9)
    rates = rates * jnp.where(hits, factor, 1.0)
    angles = jax.random.uniform(keys[3], (NE, NB, M), jnp.float32, -jnp.pi, jnp.pi)
    identity = jnp.eye(M, dtype=jnp.float32)
    diag_re = (rates * jnp.cos(angles))[..., None, :] * identity
    diag_im = (rates * jnp.sin(angles))[..., None, :] * identity
    noise = jax.random.normal(keys[4], (NE, NB, 2, M, M), jnp.float32) * (0.2 / jnp.sqrt(2.0 * M))
    return noise + jnp.stack((diag_re, diag_im), axis=2)


def levels(own_key, dims, cuts, smallest, high):
    def one(axis_at, shards_of):
        steps = jax.random.uniform(jax.random.fold_in(jax.random.fold_in(own_key, 6), axis_at), (shards_of,), jnp.float32, smallest / len(cuts), high / len(cuts))
        return jnp.repeat(jnp.exp(steps), dims[axis_at] // shards_of).reshape((-1,) + (1,) * (len(dims) - axis_at - 1))

    gain = one(*cuts[0])
    for cut in cuts[1:]:
        gain = gain * one(*cut)
    return gain


def normal_values(rng, extent, scale, reach, pieces=(), kind=jnp.bfloat16):
    array = scale * jax.random.normal(rng, extent, jnp.float32)
    if pieces:
        array = array * levels(rng, extent, pieces, -0.22, 0.18)
    return jnp.clip(array, -reach, reach).astype(kind)


def setup_inputs(seed: int = 0) -> dict:
    streams_of = jax.random.split(jax.random.key(seed), 4)
    transfer = draw_transfer(jax.random.fold_in(streams_of[3], 71), 0)
    source = normal_values(streams_of[1], (NE, NB, 2, M, M), 1.0, 6.0, ((0, 64), (1, 16)), jnp.float32)
    coulomb = normal_values(streams_of[2], (NB, M, M), 1.0, 6.0, ((0, 16),), jnp.float32)
    return {"transfer": transfer, "source": source, "coulomb": coulomb}


def matmul_high(left, right):
    return jnp.matmul(left, right, precision=lax.Precision.HIGHEST)


def complex_product(left, right):
    left_re = left[..., 0, :, :]
    left_im = left[..., 1, :, :]
    right_re = right[..., 0, :, :]
    right_im = right[..., 1, :, :]
    first = matmul_high(left_re, right_re)
    second = matmul_high(left_im, right_im)
    third = matmul_high(left_re + left_im, right_re + right_im)
    return jnp.stack((first - second, third - first - second), axis=-3)


def adjoint(matrix):
    return jnp.stack((jnp.swapaxes(matrix[..., 0, :, :], -1, -2), -jnp.swapaxes(matrix[..., 1, :, :], -1, -2)), axis=-3)


def reference(transfer, source, coulomb):
    energies = transfer.shape[0]
    order = transfer.shape[-1]

    def advance(carry, blocks):
        mapping, inject = blocks
        value = complex_product(complex_product(mapping, carry), adjoint(mapping)) + inject
        return value, value

    start = jnp.zeros((energies, 2, order, order), jnp.float32)
    _, chain = lax.scan(advance, start, (jnp.swapaxes(transfer, 0, 1), jnp.swapaxes(source, 0, 1)))

    def per_block(inputs):
        values, bare = inputs
        field = lax.complex(values[:, 0], values[:, 1])
        spectrum = jnp.fft.fft(field, n=2 * energies, axis=0)
        power = spectrum * jnp.conj(spectrum)
        lagged = jnp.fft.ifft(power, axis=0)[:energies] / energies
        polar_re = jnp.real(lagged)
        polar_im = jnp.imag(lagged)
        screen_re = bare + matmul_high(matmul_high(bare, polar_re), bare.T) / order
        screen_im = matmul_high(matmul_high(bare, polar_im), bare.T) / order
        return jnp.stack((screen_re, screen_im), axis=1)

    screened = lax.map(per_block, (chain, coulomb))
    return jnp.swapaxes(chain, 0, 1), jnp.swapaxes(screened, 0, 1)
```

```python
import functools
import math

import jax
import jax.numpy as jnp
import numpy as np
from jax import lax
from jax.experimental import pallas as pl
from jax.experimental.pallas import tpu as pltpu
from jax.sharding import Mesh
from jax.sharding import PartitionSpec as P


F32 = jnp.float32
BF16 = jnp.bfloat16
VMEM = pl.BlockSpec(memory_space=pltpu.VMEM)


def split(value):
    high = value.astype(BF16)
    return high, (value - high.astype(F32)).astype(BF16)


def put(slot, re, im):
    for n, value in enumerate((re, im, re + im, re - im)):
        slot[n, 0], slot[n, 1] = split(value)


def left(slot, n):
    return jnp.concatenate([slot[n, 0], slot[n, 0], slot[n, 1]], axis=1)


def right(slot, n):
    return jnp.concatenate([slot[n, 0], slot[n, 1], slot[n, 0]], axis=0)


def right_t(slot, n):
    return jnp.concatenate([slot[n, 0], slot[n, 1], slot[n, 0]], axis=1)


def dot(a, b):
    return jnp.dot(a, b, preferred_element_type=F32)


def dot_t(a, b):
    return lax.dot_general(a, b, (((1,), (1,)), ((), ())), preferred_element_type=F32)


def times(a, b):
    p1 = dot(left(a, 0), right(b, 0))
    p2 = dot(left(a, 1), right(b, 1))
    p3 = dot(left(a, 2), right(b, 2))
    return p1 - p2, p3 - p1 - p2


def times_adjoint(a, b):
    p1 = dot_t(left(a, 0), right_t(b, 0))
    p2 = dot_t(left(a, 1), right_t(b, 1))
    p3 = dot_t(left(a, 2), right_t(b, 3))
    return p1 + p2, p3 - p1 + p2


def sandwich(a, b, mid):
    put(mid, *times(a, b))
    return times_adjoint(mid, a)


def run(body, outs, scratch, flops, name, *args):
    many = isinstance(outs, (list, tuple))
    return pl.pallas_call(
        body,
        out_shape=outs,
        in_specs=[VMEM] * len(args),
        out_specs=[VMEM] * len(outs) if many else VMEM,
        scratch_shapes=scratch,
        compiler_params=pltpu.CompilerParams(vmem_limit_bytes=24 * 1024 * 1024),
        cost_estimate=pl.CostEstimate(flops=flops, bytes_accessed=4 << 20, transcendentals=0),
        name=name,
    )(*args)


def row_map(own, prev, opp_re, opp_im, nxt, order, prefix, total, late, *slots):
    x = lax.axis_index("ribbon_1")
    for r, ref in ((0, own), (1, prev), (3, nxt)):
        order[lax.rem(x + 4 - r, 4)] = ref[...]
    across = lax.rem(x + 2, 4)
    order[across, 0] = opp_re[...]
    order[across, 1] = opp_im[...]
    a0, a1, a2, a3, pair, upper = slots
    for j, slot in ((0, a0), (1, a1), (2, a2), (3, a3)):
        put(slot, order[j, 0], order[j, 1])
    low_re, low_im = times(a1, a0)
    up_re, up_im = times(a3, a2)
    put(pair, low_re, low_im)
    put(upper, up_re, up_im)
    late[0], late[1] = up_re, up_im
    total[0], total[1] = times(upper, pair)

    @pl.when(x == 0)
    def _():
        prefix[...] = own[...]

    @pl.when(x == 1)
    def _():
        prefix[0], prefix[1] = low_re, low_im

    @pl.when(x == 2)
    def _():
        prefix[0], prefix[1] = times(a2, pair)

    @pl.when(x == 3)
    def _():
        prefix[...] = total[...]


def row_add(order, late, own, prev, opp_re, opp_im, nxt, prefix, total, adds, *slots):
    x = lax.axis_index("ribbon_1")
    for r, ref in ((0, own), (1, prev), (3, nxt)):
        adds[lax.rem(x + 4 - r, 4)] = ref[...]
    across = lax.rem(x + 2, 4)
    adds[across, 0] = opp_re[...]
    adds[across, 1] = opp_im[...]
    a, b, c, d, mid, mid2 = slots
    put(a, order[1, 0], order[1, 1])
    put(b, adds[0, 0], adds[0, 1])
    put(c, order[3, 0], order[3, 1])
    put(d, adds[2, 0], adds[2, 1])
    low_re, low_im = sandwich(a, b, mid)
    low_re, low_im = low_re + adds[1, 0], low_im + adds[1, 1]
    up_re, up_im = sandwich(c, d, mid2)
    put(b, low_re, low_im)
    put(d, late[0], late[1])
    tot_re, tot_im = sandwich(d, b, mid)
    total[0] = tot_re + (up_re + adds[3, 0])
    total[1] = tot_im + (up_im + adds[3, 1])

    @pl.when(x == 0)
    def _():
        prefix[...] = own[...]

    @pl.when(x == 1)
    def _():
        prefix[0], prefix[1] = low_re, low_im

    @pl.when(x == 2)
    def _():
        put(a, order[2, 0], order[2, 1])
        own_re, own_im = sandwich(a, b, mid2)
        prefix[0], prefix[1] = own_re + adds[2, 0], own_im + adds[2, 1]

    @pl.when(x == 3)
    def _():
        prefix[...] = total[...]


def join_rows(pre_map, pre_add, tot_map, tot_add, got_map, got_add, joint, new_map, *slots):
    y = lax.axis_index("ribbon_0")
    a, b, mid = slots

    @pl.when(y == 0)
    def _():
        put(a, got_map[0], got_map[1])
        put(b, tot_add[0], tot_add[1])
        joint[...] = got_add[...]
        new_map[...] = pre_map[...]

    @pl.when(y == 1)
    def _():
        put(a, tot_map[0], tot_map[1])
        put(b, got_add[0], got_add[1])
        joint[...] = tot_add[...]
        new_map[...] = pre_map[...]

    @pl.when(y == 3)
    def _():
        put(b, got_map[0], got_map[1])
        put(a, pre_map[0], pre_map[1])
        new_map[0], new_map[1] = times(a, b)
        put(b, got_add[0], got_add[1])
        joint[...] = pre_add[...]

    @pl.when(y != 2)
    def _():
        re, im = sandwich(a, b, mid)
        joint[0] += re
        joint[1] += im

    @pl.when(y == 2)
    def _():
        joint[...] = pre_add[...]
        new_map[...] = pre_map[...]


def finish_chain(pre_add, joint, new_map, got_add, passed, lesser, groups, a, b, mid):
    y = lax.axis_index("ribbon_0")
    count, rows = groups.shape[0], groups.shape[3]

    @pl.when(y == 0)
    def _():
        lesser[...] = pre_add[...]

    @pl.when(y == 1)
    def _():
        put(b, got_add[0], got_add[1])
        lesser[...] = pre_add[...]

    @pl.when(y > 1)
    def _():
        put(b, passed[0], passed[1])
        lesser[...] = joint[...]

    @pl.when(y > 0)
    def _():
        put(a, new_map[0], new_map[1])
        re, im = sandwich(a, b, mid)
        lesser[0] += re
        lesser[1] += im

    for p in range(2):
        for h in range(2):
            part = lesser[p, :, h * 128 : (h + 1) * 128]
            groups[:, h, p] = part.reshape(count, rows, 128)


def correlate(forward, backward, mine, theirs, out, terms):
    c = lax.axis_index("energy_1")
    length = forward.shape[1] // 2
    count = length // 4
    rows = theirs.shape[0] // (2 * count)
    for r in range(rows):
        lanes = slice(r * 128, (r + 1) * 128)
        for p in range(2):
            own = mine[pl.ds(c * 2 * rows + p * rows + r, count, stride=4 * rows), :]
            other = theirs[pl.ds(p * rows + r, count, stride=2 * rows), :]
            for n, value in ((p, own), (2 + p, other)):
                high, low = split(value)
                terms[0, n * count : (n + 1) * count, lanes] = high
                terms[1, n * count : (n + 1) * count, lanes] = low
    table = forward[c]
    back = backward[...]
    for n in range(rows // 2):
        lanes = slice(n * 256, (n + 1) * 256)
        high, low = terms[0, :, lanes], terms[1, :, lanes]
        spec = dot(table, jnp.concatenate([high, low, high], axis=0))
        power = spec[:length] * spec[:length] + spec[length:] * spec[length:]
        high, low = split(power)
        lag = dot(back, jnp.concatenate([high, low, high], axis=0))
        for q in range(2):
            for k in range(4):
                out[pl.ds(k * rows + 2 * n + q, count, stride=4 * rows), :] = lag[
                    k * count : (k + 1) * count, q * 128 : (q + 1) * 128
                ]


def screen(bare, mine, theirs, out, both):
    c = lax.axis_index("energy_1")
    order = bare.shape[0]
    high, low = split(bare[...])
    wide = jnp.concatenate([high, high, low], axis=1)
    wide_t = jnp.concatenate([high, low, high], axis=1)
    own = [mine[:, c, p].reshape(order, 128) for p in range(2)]
    other = [theirs[:, p].reshape(order, 128) for p in range(2)]
    for at, parts in ((c, own), (1 - c, other)):
        high, low = split(jnp.concatenate(parts, axis=1))
        half = dot(wide, jnp.concatenate([high, low, high], axis=0))
        both[at, 0] = half[:, :128]
        both[at, 1] = half[:, 128:]
    for p in range(2):
        high, low = split(jnp.concatenate([both[0, p], both[1, p]], axis=1))
        full = dot_t(jnp.concatenate([high, high, low], axis=1), wide_t) * (1.0 / order)
        out[p] = bare[...] + full if p == 0 else full


def tables(energies):
    length = 2 * energies
    count = energies // 2

    def terms(table):
        high = table.astype(BF16)
        low = (table - high.astype(np.float64)).astype(BF16)
        return np.concatenate([high, high, low], axis=1)

    freq = np.arange(length)
    point = np.arange(energies)
    phase = 2.0 * math.pi / length * (np.outer(freq, point) % length)
    cosine, sine = np.cos(phase), np.sin(phase)
    forward = []
    for c in range(2):
        columns = []
        for parity in (c, 1 - c):
            co, si = cosine[:, parity::2], sine[:, parity::2]
            columns += [np.concatenate([co, -si], axis=0), np.concatenate([si, co], axis=0)]
        forward.append(terms(np.concatenate(columns, axis=1)))
    rows = []
    for parity in range(2):
        rows += [cosine.T[parity::2], sine.T[parity::2]]
    backward = terms(np.concatenate(rows, axis=0) / (length * energies))
    assert backward.shape == (4 * count, 3 * length)
    return jnp.asarray(np.stack(forward)), jnp.asarray(backward)


def shift(value, axis, step):
    length = lax.axis_size(axis)
    return lax.ppermute(value, axis, [(i, (i + step) % length) for i in range(length)])


def gather_row(value):
    prev, nxt = shift(value, "ribbon_1", 1), shift(value, "ribbon_1", -1)
    return prev, nxt


def local(transfer, source, coulomb):
    a, b, bare = transfer[0, 0], source[0, 0], coulomb[0]
    order = a.shape[-1]
    count = lax.axis_size("energy_0")
    rows = order // count
    matrix = jax.ShapeDtypeStruct((2, order, order), F32)
    slot = pltpu.VMEM((4, 2, order, order), BF16)
    product = 18 * order**3

    a_prev, a_next = gather_row(a)
    b_prev, b_next = gather_row(b)
    a_opp_re = shift(a_prev[0], "ribbon_1", 1)
    a_opp_im = shift(a_next[1], "ribbon_1", -1)
    b_opp_re = shift(b_prev[0], "ribbon_1", 1)
    b_opp_im = shift(b_next[1], "ribbon_1", -1)

    four = jax.ShapeDtypeStruct((4, 2, order, order), F32)
    maps, pre_map, tot_map, late = run(
        row_map, [four, matrix, matrix, matrix], [slot] * 6, 4 * product, "row_map",
        a, a_prev, a_opp_re, a_opp_im, a_next,
    )
    got_map = lax.ppermute(tot_map, "ribbon_0", [(1, 0), (2, 3)])
    pre_add, tot_add = run(
        row_add, [matrix, matrix], [pltpu.VMEM((4, 2, order, order), F32)] + [slot] * 6,
        8 * product, "row_add",
        maps, late, b, b_prev, b_opp_re, b_opp_im, b_next,
    )
    got_add = lax.ppermute(tot_add, "ribbon_0", [(0, 1), (1, 0), (2, 3)])
    joint, new_map = run(
        join_rows, [matrix, matrix], [slot] * 3, 3 * product, "join_rows",
        pre_map, pre_add, tot_map, tot_add, got_map, got_add,
    )
    passed = lax.ppermute(joint, "ribbon_0", [(1, 2), (0, 3)])
    lesser, groups = run(
        finish_chain,
        [matrix, jax.ShapeDtypeStruct((count, 2, 2, rows, 128), F32)],
        [slot] * 3, 2 * product, "finish_chain",
        pre_add, joint, new_map, got_add, passed,
    )

    c = lax.axis_index("energy_1")
    swap = [(0, 1), (1, 0)]
    turned = lax.all_to_all(groups.reshape(count, 4 * rows, 128), "energy_0", 0, 0, tiled=True)
    other_half = lax.dynamic_index_in_dim(
        turned.reshape(count, 2, 2 * rows, 128), 1 - c, 1, keepdims=False
    )
    theirs = lax.ppermute(other_half, "energy_1", swap)
    forward, backward = tables(2 * count)
    lags = run(
        correlate, jax.ShapeDtypeStruct((4 * count * rows, 128), F32),
        [pltpu.VMEM((2, 4 * count, rows * 128), BF16)], 4 * product, "correlate",
        forward, backward, turned.reshape(-1, 128), theirs.reshape(-1, 128),
    )
    returned = lax.all_to_all(lags.reshape(count, 4 * rows, 128), "energy_0", 0, 0, tiled=True)
    returned = returned.reshape(count, 2, 2, rows, 128)
    other_lag = lax.dynamic_index_in_dim(returned, 1 - c, 1, keepdims=False)
    halves = lax.ppermute(other_lag, "energy_1", swap)
    screened = run(
        screen, matrix, [pltpu.VMEM((2, 2, order, 128), F32)], product, "screen",
        bare, returned, halves,
    )
    return (lesser[None, None], screened[None, None])


def solution(mesh):
    sizes = (mesh.shape["energy"] // 2, 2, 4, 4)
    names = ("energy_0", "energy_1", "ribbon_0", "ribbon_1")
    split_mesh = Mesh(mesh.devices.reshape(sizes), names)
    energy, ribbon = names[:2], names[2:]
    in_specs = (
        P(energy, ribbon, None, None, None),
        P(energy, ribbon, None, None, None),
        P(ribbon, None, None),
    )
    out_specs = (P(energy, ribbon, None, None, None), P(energy, ribbon, None, None, None))
    return jax.shard_map(
        local, mesh=split_mesh, in_specs=in_specs, out_specs=out_specs, check_vma=False
    )
```

```python
import math

import jax
import jax.numpy as jnp
import numpy as np
from jax import lax
from jax.experimental import pallas as pl
from jax.experimental.pallas import tpu as pltpu
from jax.sharding import Mesh
from jax.sharding import PartitionSpec as P


F32 = jnp.float32
BF16 = jnp.bfloat16
STAGGER = 4500
VMEM = pl.BlockSpec(memory_space=pltpu.VMEM)


def split(value):
    high = value.astype(BF16)
    return high, (value - high.astype(F32)).astype(BF16)


def put(slot, re, im):
    for n, value in enumerate((re, im, re + im, re - im)):
        slot[n, 0], slot[n, 1] = split(value)


def left(slot, n):
    return jnp.concatenate([slot[n, 0], slot[n, 0], slot[n, 1]], axis=1)


def right(slot, n):
    return jnp.concatenate([slot[n, 0], slot[n, 1], slot[n, 0]], axis=0)


def right_t(slot, n):
    return jnp.concatenate([slot[n, 0], slot[n, 1], slot[n, 0]], axis=1)


def dot(a, b):
    return jnp.dot(a, b, preferred_element_type=F32)


def dot_t(a, b):
    return lax.dot_general(a, b, (((1,), (1,)), ((), ())), preferred_element_type=F32)


def times(a, b):
    p1 = dot(left(a, 0), right(b, 0))
    p2 = dot(left(a, 1), right(b, 1))
    p3 = dot(left(a, 2), right(b, 2))
    return p1 - p2, p3 - p1 - p2


def times_adjoint(a, b):
    p1 = dot_t(left(a, 0), right_t(b, 0))
    p2 = dot_t(left(a, 1), right_t(b, 1))
    p3 = dot_t(left(a, 2), right_t(b, 3))
    return p1 + p2, p3 - p1 + p2


def sandwich(a, b, mid):
    put(mid, *times(a, b))
    return times_adjoint(mid, a)


def run(body, outs, scratch, flops, *args):
    many = isinstance(outs, (list, tuple))
    return pl.pallas_call(
        body,
        out_shape=outs,
        in_specs=[VMEM] * len(args),
        out_specs=[VMEM] * len(outs) if many else VMEM,
        scratch_shapes=scratch,
        compiler_params=pltpu.CompilerParams(vmem_limit_bytes=24 * 1024 * 1024),
        cost_estimate=pl.CostEstimate(flops=flops, bytes_accessed=4 << 20, transcendentals=0),
    )(*args)


def row_map(own, prev, opp_re, opp_im, nxt, order, prefix, total, late, *slots):
    x = lax.axis_index("ribbon_1")
    for r, ref in ((0, own), (1, prev), (3, nxt)):
        order[lax.rem(x + 4 - r, 4)] = ref[...]
    across = lax.rem(x + 2, 4)
    order[across, 0] = opp_re[...]
    order[across, 1] = opp_im[...]
    a0, a1, a2, a3, pair, upper = slots
    for j, slot in ((0, a0), (1, a1), (2, a2), (3, a3)):
        put(slot, order[j, 0], order[j, 1])
    low_re, low_im = times(a1, a0)
    up_re, up_im = times(a3, a2)
    put(pair, low_re, low_im)
    put(upper, up_re, up_im)
    late[0], late[1] = up_re, up_im
    total[0], total[1] = times(upper, pair)

    @pl.when(x == 0)
    def _():
        prefix[...] = own[...]

    @pl.when(x == 1)
    def _():
        prefix[0], prefix[1] = low_re, low_im

    @pl.when(x == 2)
    def _():
        prefix[0], prefix[1] = times(a2, pair)

    @pl.when(x == 3)
    def _():
        prefix[...] = total[...]


def row_add(order, late, own, prev, opp_re, opp_im, nxt, prefix, total, adds, *slots):
    x = lax.axis_index("ribbon_1")
    for r, ref in ((0, own), (1, prev), (3, nxt)):
        adds[lax.rem(x + 4 - r, 4)] = ref[...]
    across = lax.rem(x + 2, 4)
    adds[across, 0] = opp_re[...]
    adds[across, 1] = opp_im[...]
    a, b, c, d, mid, mid2 = slots
    put(a, order[1, 0], order[1, 1])
    put(b, adds[0, 0], adds[0, 1])
    put(c, order[3, 0], order[3, 1])
    put(d, adds[2, 0], adds[2, 1])
    low_re, low_im = sandwich(a, b, mid)
    low_re, low_im = low_re + adds[1, 0], low_im + adds[1, 1]
    up_re, up_im = sandwich(c, d, mid2)
    put(b, low_re, low_im)
    put(d, late[0], late[1])
    tot_re, tot_im = sandwich(d, b, mid)
    total[0] = tot_re + (up_re + adds[3, 0])
    total[1] = tot_im + (up_im + adds[3, 1])

    @pl.when(x == 0)
    def _():
        prefix[...] = own[...]

    @pl.when(x == 1)
    def _():
        prefix[0], prefix[1] = low_re, low_im

    @pl.when(x == 2)
    def _():
        put(a, order[2, 0], order[2, 1])
        own_re, own_im = sandwich(a, b, mid2)
        prefix[0], prefix[1] = own_re + adds[2, 0], own_im + adds[2, 1]

    @pl.when(x == 3)
    def _():
        prefix[...] = total[...]


def join_rows(pre_map, pre_add, tot_map, tot_add, got_map, got_add, joint, new_map, *slots):
    y = lax.axis_index("ribbon_0")
    a, b, mid = slots

    @pl.when(y == 0)
    def _():
        put(a, got_map[0], got_map[1])
        put(b, tot_add[0], tot_add[1])
        joint[...] = got_add[...]
        new_map[...] = pre_map[...]

    @pl.when(y == 1)
    def _():
        put(a, tot_map[0], tot_map[1])
        put(b, got_add[0], got_add[1])
        joint[...] = tot_add[...]
        new_map[...] = pre_map[...]

    @pl.when(y == 3)
    def _():
        put(b, got_map[0], got_map[1])
        put(a, pre_map[0], pre_map[1])
        new_map[0], new_map[1] = times(a, b)
        put(b, got_add[0], got_add[1])
        joint[...] = pre_add[...]

    @pl.when(y != 2)
    def _():
        re, im = sandwich(a, b, mid)
        joint[0] += re
        joint[1] += im

    @pl.when(y == 2)
    def _():
        joint[...] = pre_add[...]
        new_map[...] = pre_map[...]


def finish_chain(pre_add, joint, new_map, got_add, passed, lesser, keep, send, a, b, mid):
    y = lax.axis_index("ribbon_0")
    c = lax.axis_index("energy_1")
    count, rows = keep.shape[0], keep.shape[2]

    @pl.when(y == 0)
    def _():
        lesser[...] = pre_add[...]

    @pl.when(y == 1)
    def _():
        put(b, got_add[0], got_add[1])
        lesser[...] = pre_add[...]

    @pl.when(y > 1)
    def _():
        put(b, passed[0], passed[1])
        lesser[...] = joint[...]

    @pl.when(y > 0)
    def _():
        put(a, new_map[0], new_map[1])
        re, im = sandwich(a, b, mid)
        lesser[0] += re
        lesser[1] += im

    for p in range(2):
        for half, out in ((c, keep), (1 - c, send)):
            part = lesser[p, :, pl.ds(pl.multiple_of(half * 128, 128), 128)]
            out[:, p] = part.reshape(count, rows, 128)


def pack(keep, got, groups, idle):
    c = lax.axis_index("energy_1")
    groups[:, c] = keep[...]
    groups[:, 1 - c] = got[...]

    @pl.when(c == 1)
    def _():
        idle[...] = keep[0, 0]
        idle[...] = lax.fori_loop(0, STAGGER, lambda _, v: v * 0.5 + 1.0, idle[...])


def correlate(forward, backward, given, out, terms):
    length = forward.shape[0] // 2
    count = length // 4
    rows = given.shape[0] // (4 * count)
    for r in range(rows):
        lanes = slice(r * 128, (r + 1) * 128)
        for n in range(4):
            high, low = split(given[pl.ds(n * rows + r, count, stride=4 * rows), :])
            terms[0, n * count : (n + 1) * count, lanes] = high
            terms[1, n * count : (n + 1) * count, lanes] = low
    table = forward[...]
    back = backward[...]
    for n in range(rows // 2):
        lanes = slice(n * 256, (n + 1) * 256)
        high, low = terms[0, :, lanes], terms[1, :, lanes]
        spec = dot(table, jnp.concatenate([high, low, high], axis=0))
        power = spec[:length] * spec[:length] + spec[length:] * spec[length:]
        high, low = split(power)
        lag = dot(back, jnp.concatenate([high, low, high], axis=0))
        for q in range(2):
            for k in range(4):
                out[pl.ds(k * rows + 2 * n + q, count, stride=4 * rows), :] = lag[
                    k * count : (k + 1) * count, q * 128 : (q + 1) * 128
                ]


def screen(bare, mine, theirs, out, both):
    c = lax.axis_index("energy_1")
    order = bare.shape[0]
    high, low = split(bare[...])
    wide = jnp.concatenate([high, high, low], axis=1)
    wide_t = jnp.concatenate([high, low, high], axis=1)
    own = [mine[:, c, p].reshape(order, 128) for p in range(2)]
    other = [theirs[:, p].reshape(order, 128) for p in range(2)]
    for at, parts in ((c, own), (1 - c, other)):
        high, low = split(jnp.concatenate(parts, axis=1))
        half = dot(wide, jnp.concatenate([high, low, high], axis=0))
        both[at, 0] = half[:, :128]
        both[at, 1] = half[:, 128:]
    for p in range(2):
        high, low = split(jnp.concatenate([both[0, p], both[1, p]], axis=1))
        full = dot_t(jnp.concatenate([high, high, low], axis=1), wide_t) * (1.0 / order)
        out[p] = bare[...] + full if p == 0 else full


def tables(energies):
    length = 2 * energies

    def terms(table):
        high = table.astype(BF16)
        low = (table - high.astype(np.float64)).astype(BF16)
        return np.concatenate([high, high, low], axis=1)

    freq = np.arange(length)
    point = np.arange(energies)
    phase = 2.0 * math.pi / length * (np.outer(freq, point) % length)
    cosine, sine = np.cos(phase), np.sin(phase)
    columns, rows = [], []
    for parity in range(2):
        co, si = cosine[:, parity::2], sine[:, parity::2]
        columns += [np.concatenate([co, -si], axis=0), np.concatenate([si, co], axis=0)]
        rows += [co.T, si.T]
    forward = terms(np.concatenate(columns, axis=1))
    backward = terms(np.concatenate(rows, axis=0) / (length * energies))
    return jnp.asarray(forward), jnp.asarray(backward)


def shift(value, axis, step):
    length = lax.axis_size(axis)
    return lax.ppermute(value, axis, [(i, (i + step) % length) for i in range(length)])


def gather_row(value):
    prev, nxt = shift(value, "ribbon_1", 1), shift(value, "ribbon_1", -1)
    return prev, nxt


def step(transfer, source, coulomb):
    a, b, bare = transfer[0, 0], source[0, 0], coulomb[0]
    order = a.shape[-1]
    count = lax.axis_size("energy_0")
    rows = order // count
    matrix = jax.ShapeDtypeStruct((2, order, order), F32)
    slot = pltpu.VMEM((4, 2, order, order), BF16)
    product = 18 * order**3

    a_prev, a_next = gather_row(a)
    b_prev, b_next = gather_row(b)
    a_opp_re = shift(a_prev[0], "ribbon_1", 1)
    a_opp_im = shift(a_next[1], "ribbon_1", -1)
    b_opp_re = shift(b_prev[0], "ribbon_1", 1)
    b_opp_im = shift(b_next[1], "ribbon_1", -1)

    four = jax.ShapeDtypeStruct((4, 2, order, order), F32)
    maps, pre_map, tot_map, late = run(
        row_map, [four, matrix, matrix, matrix], [slot] * 6, 4 * product,
        a, a_prev, a_opp_re, a_opp_im, a_next,
    )
    got_map = lax.ppermute(tot_map, "ribbon_0", [(1, 0), (2, 3)])
    pre_add, tot_add = run(
        row_add, [matrix, matrix], [pltpu.VMEM((4, 2, order, order), F32)] + [slot] * 6,
        8 * product,
        maps, late, b, b_prev, b_opp_re, b_opp_im, b_next,
    )
    got_add = lax.ppermute(tot_add, "ribbon_0", [(0, 1), (1, 0), (2, 3)])
    joint, new_map = run(
        join_rows, [matrix, matrix], [slot] * 3, 3 * product,
        pre_map, pre_add, tot_map, tot_add, got_map, got_add,
    )
    passed = lax.ppermute(joint, "ribbon_0", [(1, 2), (0, 3)])
    half = jax.ShapeDtypeStruct((count, 2, rows, 128), F32)
    lesser, keep, send = run(
        finish_chain, [matrix, half, half], [slot] * 3, 2 * product,
        pre_add, joint, new_map, got_add, passed,
    )

    c = lax.axis_index("energy_1")
    swap = [(0, 1), (1, 0)]
    groups = run(
        pack, jax.ShapeDtypeStruct((count, 2, 2, rows, 128), F32),
        [pltpu.VMEM((rows, 128), F32)], product,
        keep, lax.ppermute(send, "energy_1", swap),
    )
    turned = lax.all_to_all(groups.reshape(count, 4 * rows, 128), "energy_0", 0, 0, tiled=True)
    forward, backward = tables(2 * count)
    lags = run(
        correlate, jax.ShapeDtypeStruct((4 * count * rows, 128), F32),
        [pltpu.VMEM((2, 4 * count, rows * 128), BF16)], 4 * product,
        forward, backward, turned.reshape(-1, 128),
    )
    returned = lax.all_to_all(lags.reshape(count, 4 * rows, 128), "energy_0", 0, 0, tiled=True)
    returned = returned.reshape(count, 2, 2, rows, 128)
    other_lag = lax.dynamic_index_in_dim(returned, 1 - c, 1, keepdims=False)
    halves = lax.ppermute(other_lag, "energy_1", swap)
    screened = run(
        screen, matrix, [pltpu.VMEM((2, 2, order, 128), F32)], product,
        bare, returned, halves,
    )
    return (lesser[None, None], screened[None, None])


def solution(mesh):
    sizes = (mesh.shape["energy"] // 2, 2, 4, 4)
    names = ("energy_0", "energy_1", "ribbon_0", "ribbon_1")
    split_mesh = Mesh(mesh.devices.reshape(sizes), names)
    energy, ribbon = names[:2], names[2:]
    in_specs = (
        P(energy, ribbon, None, None, None),
        P(energy, ribbon, None, None, None),
        P(ribbon, None, None),
    )
    out_specs = (P(energy, ribbon, None, None, None), P(energy, ribbon, None, None, None))
    return jax.shard_map(
        step, mesh=split_mesh, in_specs=in_specs, out_specs=out_specs, check_vma=False
    )
```

```python
import math

import jax
import jax.numpy as jnp
import numpy as np
from jax import lax
from jax.experimental import pallas as pl
from jax.experimental.pallas import tpu as pltpu
from jax.sharding import Mesh
from jax.sharding import PartitionSpec as P


F32 = jnp.float32
BF16 = jnp.bfloat16
STAGGER = 4400
LEAD = 2000
VMEM = pl.BlockSpec(memory_space=pltpu.VMEM)


def split(value):
    high = value.astype(BF16)
    return high, (value - high.astype(F32)).astype(BF16)


def put(slot, re, im):
    for n, value in enumerate((re, im, re + im, re - im)):
        slot[n, 0], slot[n, 1] = split(value)


def left(slot, n):
    return jnp.concatenate([slot[n, 0], slot[n, 0], slot[n, 1]], axis=1)


def right(slot, n):
    return jnp.concatenate([slot[n, 0], slot[n, 1], slot[n, 0]], axis=0)


def right_t(slot, n):
    return jnp.concatenate([slot[n, 0], slot[n, 1], slot[n, 0]], axis=1)


def dot(a, b):
    return jnp.dot(a, b, preferred_element_type=F32)


def dot_t(a, b):
    return lax.dot_general(a, b, (((1,), (1,)), ((), ())), preferred_element_type=F32)


def times(a, b):
    p1 = dot(left(a, 0), right(b, 0))
    p2 = dot(left(a, 1), right(b, 1))
    p3 = dot(left(a, 2), right(b, 2))
    return p1 - p2, p3 - p1 - p2


def times_adjoint(a, b):
    p1 = dot_t(left(a, 0), right_t(b, 0))
    p2 = dot_t(left(a, 1), right_t(b, 1))
    p3 = dot_t(left(a, 2), right_t(b, 3))
    return p1 + p2, p3 - p1 + p2


def sandwich(a, b, mid):
    put(mid, *times(a, b))
    return times_adjoint(mid, a)


def run(body, outs, scratch, flops, *args):
    many = isinstance(outs, (list, tuple))
    return pl.pallas_call(
        body,
        out_shape=outs,
        in_specs=[VMEM] * len(args),
        out_specs=[VMEM] * len(outs) if many else VMEM,
        scratch_shapes=scratch,
        compiler_params=pltpu.CompilerParams(vmem_limit_bytes=24 * 1024 * 1024),
        cost_estimate=pl.CostEstimate(flops=flops, bytes_accessed=4 << 20, transcendentals=0),
    )(*args)


def row_map(own, prev, opp, nxt, order, prefix, total, late, *slots):
    x = lax.axis_index("ribbon_1")
    for r, ref in enumerate((own, prev, opp, nxt)):
        order[lax.rem(x + 4 - r, 4)] = ref[...]
    a0, a1, a2, a3, pair, upper = slots
    for j, slot in ((0, a0), (1, a1), (2, a2), (3, a3)):
        put(slot, order[j, 0], order[j, 1])
    low_re, low_im = times(a1, a0)
    up_re, up_im = times(a3, a2)
    put(pair, low_re, low_im)
    put(upper, up_re, up_im)
    late[0], late[1] = up_re, up_im
    total[0], total[1] = times(upper, pair)

    @pl.when(x == 0)
    def _():
        prefix[...] = own[...]

    @pl.when(x == 1)
    def _():
        prefix[0], prefix[1] = low_re, low_im

    @pl.when(x == 2)
    def _():
        prefix[0], prefix[1] = times(a2, pair)

    @pl.when(x == 3)
    def _():
        prefix[...] = total[...]


def row_add(order, late, own, prev, opp, nxt, prefix, total, adds, *slots):
    x = lax.axis_index("ribbon_1")
    for r, ref in enumerate((own, prev, opp, nxt)):
        adds[lax.rem(x + 4 - r, 4)] = ref[...]
    a, b, c, d, mid, mid2 = slots
    put(a, order[1, 0], order[1, 1])
    put(b, adds[0, 0], adds[0, 1])
    put(c, order[3, 0], order[3, 1])
    put(d, adds[2, 0], adds[2, 1])
    low_re, low_im = sandwich(a, b, mid)
    low_re, low_im = low_re + adds[1, 0], low_im + adds[1, 1]
    up_re, up_im = sandwich(c, d, mid2)
    put(b, low_re, low_im)
    put(d, late[0], late[1])
    tot_re, tot_im = sandwich(d, b, mid)
    total[0] = tot_re + (up_re + adds[3, 0])
    total[1] = tot_im + (up_im + adds[3, 1])

    @pl.when(x == 0)
    def _():
        prefix[...] = own[...]

    @pl.when(x == 1)
    def _():
        prefix[0], prefix[1] = low_re, low_im

    @pl.when(x == 2)
    def _():
        put(a, order[2, 0], order[2, 1])
        own_re, own_im = sandwich(a, b, mid2)
        prefix[0], prefix[1] = own_re + adds[2, 0], own_im + adds[2, 1]

    @pl.when(x == 3)
    def _():
        prefix[...] = total[...]


def join_rows(pre_map, pre_add, tot_map, tot_add, got_map, got_add, joint, new_map, *slots):
    y = lax.axis_index("ribbon_0")
    a, b, mid = slots

    @pl.when(y == 0)
    def _():
        put(a, got_map[0], got_map[1])
        put(b, tot_add[0], tot_add[1])
        joint[...] = got_add[...]
        new_map[...] = pre_map[...]

    @pl.when(y == 1)
    def _():
        put(a, tot_map[0], tot_map[1])
        put(b, got_add[0], got_add[1])
        joint[...] = tot_add[...]
        new_map[...] = pre_map[...]

    @pl.when(y == 3)
    def _():
        put(b, got_map[0], got_map[1])
        put(a, pre_map[0], pre_map[1])
        new_map[0], new_map[1] = times(a, b)
        put(b, got_add[0], got_add[1])
        joint[...] = pre_add[...]

    @pl.when(y != 2)
    def _():
        re, im = sandwich(a, b, mid)
        joint[0] += re
        joint[1] += im

    @pl.when(y == 2)
    def _():
        joint[...] = pre_add[...]
        new_map[...] = pre_map[...]


def finish_chain(pre_add, joint, new_map, got_add, passed, lesser, keep, send, a, b, mid):
    y = lax.axis_index("ribbon_0")
    c = lax.axis_index("energy_1")
    count, rows = keep.shape[0], keep.shape[2]

    @pl.when(y == 0)
    def _():
        lesser[...] = pre_add[...]

    @pl.when(y == 1)
    def _():
        put(b, got_add[0], got_add[1])
        lesser[...] = pre_add[...]

    @pl.when(y > 1)
    def _():
        put(b, passed[0], passed[1])
        lesser[...] = joint[...]

    @pl.when(y > 0)
    def _():
        put(a, new_map[0], new_map[1])
        re, im = sandwich(a, b, mid)
        lesser[0] += re
        lesser[1] += im

    for p in range(2):
        for half, out in ((c, keep), (1 - c, send)):
            part = lesser[p, :, pl.ds(pl.multiple_of(half * 128, 128), 128)]
            out[:, p] = part.reshape(count, rows, 128)


def core_waits(core, steps, idle):
    @pl.when(lax.axis_index("energy_1") == core)
    def _():
        idle[...] = jnp.zeros_like(idle)
        idle[...] = lax.fori_loop(0, steps, lambda _, v: v * 0.5 + 1.0, idle[...])


def hold(idle):
    core_waits(1, LEAD, idle)


def pack(keep, got, groups, idle):
    c = lax.axis_index("energy_1")
    groups[:, c] = keep[...]
    groups[:, 1 - c] = got[...]
    core_waits(0, STAGGER, idle)


def correlate(forward, backward, given, out, terms):
    length = forward.shape[0] // 2
    count = length // 4
    rows = given.shape[0] // (4 * count)
    for r in range(rows):
        lanes = slice(r * 128, (r + 1) * 128)
        for n in range(4):
            high, low = split(given[pl.ds(n * rows + r, count, stride=4 * rows), :])
            terms[0, n * count : (n + 1) * count, lanes] = high
            terms[1, n * count : (n + 1) * count, lanes] = low
    table = forward[...]
    back = backward[...]
    for n in range(rows // 2):
        lanes = slice(n * 256, (n + 1) * 256)
        high, low = terms[0, :, lanes], terms[1, :, lanes]
        spec = dot(table, jnp.concatenate([high, low, high], axis=0))
        power = spec[:length] * spec[:length] + spec[length:] * spec[length:]
        high, low = split(power)
        lag = dot(back, jnp.concatenate([high, low, high], axis=0))
        for q in range(2):
            for k in range(4):
                out[pl.ds(k * rows + 2 * n + q, count, stride=4 * rows), :] = lag[
                    k * count : (k + 1) * count, q * 128 : (q + 1) * 128
                ]


def screen(bare, mine, theirs, out, both):
    c = lax.axis_index("energy_1")
    order = bare.shape[0]
    high, low = split(bare[...])
    wide = jnp.concatenate([high, high, low], axis=1)
    wide_t = jnp.concatenate([high, low, high], axis=1)
    own = [mine[:, c, p].reshape(order, 128) for p in range(2)]
    other = [theirs[:, p].reshape(order, 128) for p in range(2)]
    for at, parts in ((c, own), (1 - c, other)):
        high, low = split(jnp.concatenate(parts, axis=1))
        half = dot(wide, jnp.concatenate([high, low, high], axis=0))
        both[at, 0] = half[:, :128]
        both[at, 1] = half[:, 128:]
    for p in range(2):
        high, low = split(jnp.concatenate([both[0, p], both[1, p]], axis=1))
        full = dot_t(jnp.concatenate([high, high, low], axis=1), wide_t) * (1.0 / order)
        out[p] = bare[...] + full if p == 0 else full


def tables(energies):
    length = 2 * energies

    def terms(table):
        high = table.astype(BF16)
        low = (table - high.astype(np.float64)).astype(BF16)
        return np.concatenate([high, high, low], axis=1)

    freq = np.arange(length)
    point = np.arange(energies)
    phase = 2.0 * math.pi / length * (np.outer(freq, point) % length)
    cosine, sine = np.cos(phase), np.sin(phase)
    columns, rows = [], []
    for parity in range(2):
        co, si = cosine[:, parity::2], sine[:, parity::2]
        columns += [np.concatenate([co, -si], axis=0), np.concatenate([si, co], axis=0)]
        rows += [co.T, si.T]
    forward = terms(np.concatenate(columns, axis=1))
    backward = terms(np.concatenate(rows, axis=0) / (length * energies))
    return jnp.asarray(forward), jnp.asarray(backward)


def shift(value, axis, step):
    length = lax.axis_size(axis)
    return lax.ppermute(value, axis, [(i, (i + step) % length) for i in range(length)])


def step(transfer, source, coulomb):
    a, b, bare = transfer[0, 0], source[0, 0], coulomb[0]
    order = a.shape[-1]
    count = lax.axis_size("energy_0")
    rows = order // count
    matrix = jax.ShapeDtypeStruct((2, order, order), F32)
    slot = pltpu.VMEM((4, 2, order, order), BF16)
    product = 18 * order**3

    pl.pallas_call(
        hold, out_shape=jax.ShapeDtypeStruct((8, 128), F32), out_specs=VMEM, name="hold",
        compiler_params=pltpu.CompilerParams(has_side_effects=True),
    )()
    a_prev = shift(a, "ribbon_1", 1)
    b_next = shift(b, "ribbon_1", -1)
    b_prev = shift(b, "ribbon_1", 1)
    a_next = shift(a, "ribbon_1", -1)
    a_opp = shift(a_prev, "ribbon_1", 1)
    b_opp = shift(b_next, "ribbon_1", -1)

    four = jax.ShapeDtypeStruct((4, 2, order, order), F32)
    maps, pre_map, tot_map, late = run(
        row_map, [four, matrix, matrix, matrix], [slot] * 6, 4 * product,
        a, a_prev, a_opp, a_next,
    )
    got_map = lax.ppermute(tot_map, "ribbon_0", [(1, 0), (2, 3)])
    pre_add, tot_add = run(
        row_add, [matrix, matrix], [pltpu.VMEM((4, 2, order, order), F32)] + [slot] * 6,
        8 * product,
        maps, late, b, b_prev, b_opp, b_next,
    )
    got_add = lax.ppermute(tot_add, "ribbon_0", [(0, 1), (1, 0), (2, 3)])
    joint, new_map = run(
        join_rows, [matrix, matrix], [slot] * 3, 3 * product,
        pre_map, pre_add, tot_map, tot_add, got_map, got_add,
    )
    passed = lax.ppermute(joint, "ribbon_0", [(1, 2), (0, 3)])
    half = jax.ShapeDtypeStruct((count, 2, rows, 128), F32)
    lesser, keep, send = run(
        finish_chain, [matrix, half, half], [slot] * 3, 2 * product,
        pre_add, joint, new_map, got_add, passed,
    )

    c = lax.axis_index("energy_1")
    swap = [(0, 1), (1, 0)]
    groups = run(
        pack, jax.ShapeDtypeStruct((count, 2, 2, rows, 128), F32),
        [pltpu.VMEM((rows, 128), F32)], product,
        keep, lax.ppermute(send, "energy_1", swap),
    )
    turned = lax.all_to_all(groups.reshape(count, 4 * rows, 128), "energy_0", 0, 0, tiled=True)
    forward, backward = tables(2 * count)
    lags = run(
        correlate, jax.ShapeDtypeStruct((4 * count * rows, 128), F32),
        [pltpu.VMEM((2, 4 * count, rows * 128), BF16)], 4 * product,
        forward, backward, turned.reshape(-1, 128),
    )
    returned = lax.all_to_all(lags.reshape(count, 4 * rows, 128), "energy_0", 0, 0, tiled=True)
    returned = returned.reshape(count, 2, 2, rows, 128)
    other_lag = lax.dynamic_index_in_dim(returned, 1 - c, 1, keepdims=False)
    halves = lax.ppermute(other_lag, "energy_1", swap)
    screened = run(
        screen, matrix, [pltpu.VMEM((2, 2, order, 128), F32)], product,
        bare, returned, halves,
    )
    return (lesser[None, None], screened[None, None])


def solution(mesh):
    sizes = (mesh.shape["energy"] // 2, 2, 4, 4)
    names = ("energy_0", "energy_1", "ribbon_0", "ribbon_1")
    split_mesh = Mesh(mesh.devices.reshape(sizes), names)
    energy, ribbon = names[:2], names[2:]
    in_specs = (
        P(energy, ribbon, None, None, None),
        P(energy, ribbon, None, None, None),
        P(ribbon, None, None),
    )
    out_specs = (P(energy, ribbon, None, None, None), P(energy, ribbon, None, None, None))
    return jax.shard_map(
        step, mesh=split_mesh, in_specs=in_specs, out_specs=out_specs, check_vma=False
    )
```

```python
import math

import jax
import jax.numpy as jnp
import numpy as np
from jax import lax
from jax.experimental import pallas as pl
from jax.experimental.pallas import tpu as pltpu
from jax.sharding import Mesh
from jax.sharding import PartitionSpec as P


F32 = jnp.float32
BF16 = jnp.bfloat16
STAGGER = 4200
LEAD = 2500
VMEM = pl.BlockSpec(memory_space=pltpu.VMEM)


def split(value):
    high = value.astype(BF16)
    return high, (value - high.astype(F32)).astype(BF16)


def put(slot, re, im):
    for n, value in enumerate((re, im, re + im, re - im)):
        slot[n, 0], slot[n, 1] = split(value)


def left(slot, n):
    return jnp.concatenate([slot[n, 0], slot[n, 0], slot[n, 1]], axis=1)


def right(slot, n):
    return jnp.concatenate([slot[n, 0], slot[n, 1], slot[n, 0]], axis=0)


def right_t(slot, n):
    return jnp.concatenate([slot[n, 0], slot[n, 1], slot[n, 0]], axis=1)


def dot(a, b):
    return jnp.dot(a, b, preferred_element_type=F32)


def dot_t(a, b):
    return lax.dot_general(a, b, (((1,), (1,)), ((), ())), preferred_element_type=F32)


def times(a, b):
    p1 = dot(left(a, 0), right(b, 0))
    p2 = dot(left(a, 1), right(b, 1))
    p3 = dot(left(a, 2), right(b, 2))
    return p1 - p2, p3 - p1 - p2


def times_adjoint(a, b):
    p1 = dot_t(left(a, 0), right_t(b, 0))
    p2 = dot_t(left(a, 1), right_t(b, 1))
    p3 = dot_t(left(a, 2), right_t(b, 3))
    return p1 + p2, p3 - p1 + p2


def sandwich(a, b, mid):
    put(mid, *times(a, b))
    return times_adjoint(mid, a)


def run(body, outs, scratch, flops, *args):
    many = isinstance(outs, (list, tuple))
    return pl.pallas_call(
        body,
        out_shape=outs,
        in_specs=[VMEM] * len(args),
        out_specs=[VMEM] * len(outs) if many else VMEM,
        scratch_shapes=scratch,
        compiler_params=pltpu.CompilerParams(vmem_limit_bytes=24 * 1024 * 1024),
        cost_estimate=pl.CostEstimate(flops=flops, bytes_accessed=4 << 20, transcendentals=0),
    )(*args)


def row_map(own, prev, opp, nxt, order, prefix, total, late, *slots):
    x = lax.axis_index("ribbon_1")
    for r, ref in enumerate((own, prev, opp, nxt)):
        order[lax.rem(x + 4 - r, 4)] = ref[...]
    a0, a1, a2, a3, pair, upper = slots
    for j, slot in ((0, a0), (1, a1), (2, a2), (3, a3)):
        put(slot, order[j, 0], order[j, 1])
    low_re, low_im = times(a1, a0)
    up_re, up_im = times(a3, a2)
    put(pair, low_re, low_im)
    put(upper, up_re, up_im)
    late[0], late[1] = up_re, up_im
    total[0], total[1] = times(upper, pair)

    @pl.when(x == 0)
    def _():
        prefix[...] = own[...]

    @pl.when(x == 1)
    def _():
        prefix[0], prefix[1] = low_re, low_im

    @pl.when(x == 2)
    def _():
        prefix[0], prefix[1] = times(a2, pair)

    @pl.when(x == 3)
    def _():
        prefix[...] = total[...]


def row_add(order, late, own, prev, opp, nxt, prefix, total, adds, *slots):
    x = lax.axis_index("ribbon_1")
    for r, ref in enumerate((own, prev, opp, nxt)):
        adds[lax.rem(x + 4 - r, 4)] = ref[...]
    a, b, c, d, mid, mid2 = slots
    put(a, order[1, 0], order[1, 1])
    put(b, adds[0, 0], adds[0, 1])
    put(c, order[3, 0], order[3, 1])
    put(d, adds[2, 0], adds[2, 1])
    low_re, low_im = sandwich(a, b, mid)
    low_re, low_im = low_re + adds[1, 0], low_im + adds[1, 1]
    up_re, up_im = sandwich(c, d, mid2)
    put(b, low_re, low_im)
    put(d, late[0], late[1])
    tot_re, tot_im = sandwich(d, b, mid)
    total[0] = tot_re + (up_re + adds[3, 0])
    total[1] = tot_im + (up_im + adds[3, 1])

    @pl.when(x == 0)
    def _():
        prefix[...] = own[...]

    @pl.when(x == 1)
    def _():
        prefix[0], prefix[1] = low_re, low_im

    @pl.when(x == 2)
    def _():
        put(a, order[2, 0], order[2, 1])
        own_re, own_im = sandwich(a, b, mid2)
        prefix[0], prefix[1] = own_re + adds[2, 0], own_im + adds[2, 1]

    @pl.when(x == 3)
    def _():
        prefix[...] = total[...]


def join_rows(pre_map, pre_add, tot_map, tot_add, got_map, got_add, joint, new_map, *slots):
    y = lax.axis_index("ribbon_0")
    a, b, mid = slots

    @pl.when(y == 0)
    def _():
        put(a, got_map[0], got_map[1])
        put(b, tot_add[0], tot_add[1])
        joint[...] = got_add[...]
        new_map[...] = pre_map[...]

    @pl.when(y == 1)
    def _():
        put(a, tot_map[0], tot_map[1])
        put(b, got_add[0], got_add[1])
        joint[...] = tot_add[...]
        new_map[...] = pre_map[...]

    @pl.when(y == 3)
    def _():
        put(b, got_map[0], got_map[1])
        put(a, pre_map[0], pre_map[1])
        new_map[0], new_map[1] = times(a, b)
        put(b, got_add[0], got_add[1])
        joint[...] = pre_add[...]

    @pl.when(y != 2)
    def _():
        re, im = sandwich(a, b, mid)
        joint[0] += re
        joint[1] += im

    @pl.when(y == 2)
    def _():
        joint[...] = pre_add[...]
        new_map[...] = pre_map[...]


def finish_chain(pre_add, joint, new_map, got_add, passed, lesser, keep, send, a, b, mid):
    y = lax.axis_index("ribbon_0")
    c = lax.axis_index("energy_1")
    count, rows = keep.shape[0], keep.shape[2]

    @pl.when(y == 0)
    def _():
        lesser[...] = pre_add[...]

    @pl.when(y == 1)
    def _():
        put(b, got_add[0], got_add[1])
        lesser[...] = pre_add[...]

    @pl.when(y > 1)
    def _():
        put(b, passed[0], passed[1])
        lesser[...] = joint[...]

    @pl.when(y > 0)
    def _():
        put(a, new_map[0], new_map[1])
        re, im = sandwich(a, b, mid)
        lesser[0] += re
        lesser[1] += im

    for p in range(2):
        for half, out in ((c, keep), (1 - c, send)):
            part = lesser[p, :, pl.ds(pl.multiple_of(half * 128, 128), 128)]
            out[:, p] = part.reshape(count, rows, 128)


def core_waits(core, steps, idle):
    @pl.when(lax.axis_index("energy_1") == core)
    def _():
        idle[...] = jnp.zeros_like(idle)
        idle[...] = lax.fori_loop(0, steps, lambda _, v: v * 0.5 + 1.0, idle[...])


def hold(idle):
    core_waits(1, LEAD, idle)


def pack(keep, got, groups, idle):
    c = lax.axis_index("energy_1")
    groups[:, c] = keep[...]
    groups[:, 1 - c] = got[...]
    core_waits(0, STAGGER, idle)


def correlate(forward, backward, given, out, terms):
    length = forward.shape[0] // 2
    count = length // 4
    rows = given.shape[0] // (4 * count)
    for r in range(rows):
        lanes = slice(r * 128, (r + 1) * 128)
        for n in range(4):
            high, low = split(given[pl.ds(n * rows + r, count, stride=4 * rows), :])
            terms[0, n * count : (n + 1) * count, lanes] = high
            terms[1, n * count : (n + 1) * count, lanes] = low
    table = forward[...]
    back = backward[...]
    for n in range(rows // 2):
        lanes = slice(n * 256, (n + 1) * 256)
        high, low = terms[0, :, lanes], terms[1, :, lanes]
        spec = dot(table, jnp.concatenate([high, low, high], axis=0))
        power = spec[:length] * spec[:length] + spec[length:] * spec[length:]
        high, low = split(power)
        lag = dot(back, jnp.concatenate([high, low, high], axis=0))
        for q in range(2):
            for k in range(4):
                out[pl.ds(k * rows + 2 * n + q, count, stride=4 * rows), :] = lag[
                    k * count : (k + 1) * count, q * 128 : (q + 1) * 128
                ]


def bare_times(bare, parts):
    high, low = split(bare)
    wide = jnp.concatenate([high, high, low], axis=1)
    high, low = split(jnp.concatenate(parts, axis=1))
    half = dot(wide, jnp.concatenate([high, low, high], axis=0))
    return half[:, :128], half[:, 128:]


def screen_own(bare, mine, out):
    c = lax.axis_index("energy_1")
    order = bare.shape[0]
    parts = [mine[:, c, p].reshape(order, 128) for p in range(2)]
    out[0], out[1] = bare_times(bare[...], parts)


def screen(bare, own, theirs, out, both):
    c = lax.axis_index("energy_1")
    order = bare.shape[0]
    both[c] = own[...]
    parts = [theirs[:, p].reshape(order, 128) for p in range(2)]
    both[1 - c, 0], both[1 - c, 1] = bare_times(bare[...], parts)
    high, low = split(bare[...])
    wide = jnp.concatenate([high, low, high], axis=1)
    for p in range(2):
        high, low = split(jnp.concatenate([both[0, p], both[1, p]], axis=1))
        full = dot_t(jnp.concatenate([high, high, low], axis=1), wide) * (1.0 / order)
        out[p] = bare[...] + full if p == 0 else full


def tables(energies):
    length = 2 * energies

    def terms(table):
        high = table.astype(BF16)
        low = (table - high.astype(np.float64)).astype(BF16)
        return np.concatenate([high, high, low], axis=1)

    freq = np.arange(length)
    point = np.arange(energies)
    phase = 2.0 * math.pi / length * (np.outer(freq, point) % length)
    cosine, sine = np.cos(phase), np.sin(phase)
    columns, rows = [], []
    for parity in range(2):
        co, si = cosine[:, parity::2], sine[:, parity::2]
        columns += [np.concatenate([co, -si], axis=0), np.concatenate([si, co], axis=0)]
        rows += [co.T, si.T]
    forward = terms(np.concatenate(columns, axis=1))
    backward = terms(np.concatenate(rows, axis=0) / (length * energies))
    return jnp.asarray(forward), jnp.asarray(backward)


def shift(value, axis, step):
    length = lax.axis_size(axis)
    return lax.ppermute(value, axis, [(i, (i + step) % length) for i in range(length)])


def step(transfer, source, coulomb):
    a, b, bare = transfer[0, 0], source[0, 0], coulomb[0]
    order = a.shape[-1]
    count = lax.axis_size("energy_0")
    rows = order // count
    matrix = jax.ShapeDtypeStruct((2, order, order), F32)
    slot = pltpu.VMEM((4, 2, order, order), BF16)
    product = 18 * order**3

    pl.pallas_call(
        hold, out_shape=jax.ShapeDtypeStruct((8, 128), F32), out_specs=VMEM, name="hold",
        compiler_params=pltpu.CompilerParams(has_side_effects=True),
    )()
    a_prev = shift(a, "ribbon_1", 1)
    b_next = shift(b, "ribbon_1", -1)
    b_prev = shift(b, "ribbon_1", 1)
    a_next = shift(a, "ribbon_1", -1)
    a_opp = shift(a_prev, "ribbon_1", 1)
    b_opp = shift(b_next, "ribbon_1", -1)

    four = jax.ShapeDtypeStruct((4, 2, order, order), F32)
    maps, pre_map, tot_map, late = run(
        row_map, [four, matrix, matrix, matrix], [slot] * 6, 4 * product,
        a, a_prev, a_opp, a_next,
    )
    got_map = lax.ppermute(tot_map, "ribbon_0", [(1, 0), (2, 3)])
    pre_add, tot_add = run(
        row_add, [matrix, matrix], [pltpu.VMEM((4, 2, order, order), F32)] + [slot] * 6,
        8 * product,
        maps, late, b, b_prev, b_opp, b_next,
    )
    got_add = lax.ppermute(tot_add, "ribbon_0", [(0, 1), (1, 0), (2, 3)])
    joint, new_map = run(
        join_rows, [matrix, matrix], [slot] * 3, 3 * product,
        pre_map, pre_add, tot_map, tot_add, got_map, got_add,
    )
    passed = lax.ppermute(joint, "ribbon_0", [(1, 2), (0, 3)])
    half = jax.ShapeDtypeStruct((count, 2, rows, 128), F32)
    lesser, keep, send = run(
        finish_chain, [matrix, half, half], [slot] * 3, 2 * product,
        pre_add, joint, new_map, got_add, passed,
    )

    c = lax.axis_index("energy_1")
    swap = [(0, 1), (1, 0)]
    groups = run(
        pack, jax.ShapeDtypeStruct((count, 2, 2, rows, 128), F32),
        [pltpu.VMEM((rows, 128), F32)], product,
        keep, lax.ppermute(send, "energy_1", swap),
    )
    turned = lax.all_to_all(groups.reshape(count, 4 * rows, 128), "energy_0", 0, 0, tiled=True)
    forward, backward = tables(2 * count)
    lags = run(
        correlate, jax.ShapeDtypeStruct((4 * count * rows, 128), F32),
        [pltpu.VMEM((2, 4 * count, rows * 128), BF16)], 4 * product,
        forward, backward, turned.reshape(-1, 128),
    )
    returned = lax.all_to_all(lags.reshape(count, 4 * rows, 128), "energy_0", 0, 0, tiled=True)
    returned = returned.reshape(count, 2, 2, rows, 128)
    other_lag = lax.dynamic_index_in_dim(returned, 1 - c, 1, keepdims=False)
    halves = lax.ppermute(other_lag, "energy_1", swap)
    own_part = run(
        screen_own, jax.ShapeDtypeStruct((2, order, 128), F32), [], product,
        bare, returned,
    )
    screened = run(
        screen, matrix, [pltpu.VMEM((2, 2, order, 128), F32)], product,
        bare, own_part, halves,
    )
    return (lesser[None, None], screened[None, None])


def solution(mesh):
    sizes = (mesh.shape["energy"] // 2, 2, 4, 4)
    names = ("energy_0", "energy_1", "ribbon_0", "ribbon_1")
    split_mesh = Mesh(mesh.devices.reshape(sizes), names)
    energy, ribbon = names[:2], names[2:]
    in_specs = (
        P(energy, ribbon, None, None, None),
        P(energy, ribbon, None, None, None),
        P(ribbon, None, None),
    )
    out_specs = (P(energy, ribbon, None, None, None), P(energy, ribbon, None, None, None))
    return jax.shard_map(
        step, mesh=split_mesh, in_specs=in_specs, out_specs=out_specs, check_vma=False
    )
```
